32 devices in a mesh: dp: 2 (over x), tp: 4 (over z), sp: 4 (over y, core).
Axes of the slice: x: 2, y: 2, z: 4, core: 2. Of those that a mesh axis runs over, the one named last changes fastest.
Arguments:
- hidden: bfloat16 [128, 8192], P('dp'), parts along dimension 0
- seq_lens: int32 [128], P('dp'), parts along dimension 0
- rope_cos: float32 [128, 64], P('dp'), parts along dimension 0
- rope_sin: float32 [128, 64], P('dp'), parts along dimension 0
- k_cache: bfloat16 [128, 256, 8, 128], P('dp', 'sp', 'tp'), parts along dimension 0
- v_cache: bfloat16 [128, 256, 8, 128], P('dp', 'sp', 'tp'), parts along dimension 0
- norm_gain: bfloat16 [8192], replicated
- w_qkv: bfloat16 [8192, 8, 1280], P(None, 'tp')
- b_qkv: bfloat16 [8, 1280], P('tp')
- sink_logits: float32 [64], P('tp')
- w_o: bfloat16 [8192, 8192], P('tp')
- b_o: bfloat16 [8192], replicated
Outputs:
- output 1: bfloat16 [128, 8192], P('dp'), parts along dimension 0
- output 2: bfloat16 [128, 256, 8, 128], P('dp', 'sp', 'tp'), parts along dimension 0
- output 3: bfloat16 [128, 256, 8, 128], P('dp', 'sp', 'tp'), parts along dimension 0
There are 2 independent parts. The reference program is written for one: setup_inputs(seed, part) draws one part's arguments, and reference() takes and returns one part's arrays. A program takes and returns all parts, laid end to end along the dimension named above; an argument that names none is the same for every part.
All inputs are finite; a program needn't handle non-finite values.
Results may differ from the reference program's by a relative error of at most 0.00542463.
Values sent between devices are 32-bit elements.
A program may use at most 1 GiB of HBM per device.

```python
import math
import jax
import jax.numpy as jnp
from jax import lax

D_MODEL = 8192
Q_HEADS = 64
KV_HEADS = 8
HEAD_DIM = 128
SEQ_COUNT = 64
CTX_LEN = 256
ROPE_BASE = 150000
NORM_EPS = 1e-5


def rotate_half(heads_in, cos_part, sin_part):
    half_dim = heads_in.shape[-1] // 2
    first_half = heads_in[..., :half_dim]
    second_half = heads_in[..., half_dim:]
    return jnp.concatenate([first_half * cos_part - second_half * sin_part, second_half * cos_part + first_half * sin_part], axis=-1)


def setup_inputs(seed: int = 0, part: int = 0) -> dict:
    shared_keys = jax.random.split(jax.random.key(seed), 6)
    part_keys = jax.random.split(jax.random.fold_in(jax.random.key(seed + 1), part), 5)
    group_size = Q_HEADS // KV_HEADS
    qkv_width = (group_size + 2) * HEAD_DIM
    key_scale = math.sqrt(math.log(CTX_LEN) / 2.0)
    sink_center = math.log(CTX_LEN / 2.0) + 0.6 * key_scale * key_scale - 1.0
    hidden = (0.5 * jax.random.normal(part_keys[0], (SEQ_COUNT, D_MODEL), jnp.float32)).astype(jnp.bfloat16)
    drawn_lens = jax.random.randint(part_keys[1], (SEQ_COUNT,), 0, CTX_LEN, jnp.int32)
    full_row = jax.random.randint(part_keys[2], (), 0, SEQ_COUNT, jnp.int32)
    seq_lens = jnp.where(jnp.arange(SEQ_COUNT) == full_row, CTX_LEN - 1, drawn_lens).astype(jnp.int32)
    inv_freq = jnp.exp(jnp.arange(HEAD_DIM // 2, dtype=jnp.float32) * (-2.0 * math.log(ROPE_BASE) / HEAD_DIM))
    angles = seq_lens.astype(jnp.float32)[:, None] * inv_freq[None, :]
    cache_shape = (SEQ_COUNT, CTX_LEN, KV_HEADS, HEAD_DIM)
    k_cache = (key_scale * jax.random.normal(part_keys[3], cache_shape, jnp.float32)).astype(jnp.bfloat16)
    v_cache = jax.random.normal(part_keys[4], cache_shape, jnp.float32).astype(jnp.bfloat16)
    norm_gain = (1.0 + 0.2 * jax.random.normal(shared_keys[0], (D_MODEL,), jnp.float32)).astype(jnp.bfloat16)
    w_qkv = (D_MODEL ** -0.5 * jax.random.normal(shared_keys[1], (D_MODEL, KV_HEADS, qkv_width), jnp.float32)).astype(jnp.bfloat16)
    b_qkv = (0.5 * jax.random.normal(shared_keys[2], (KV_HEADS, qkv_width), jnp.float32)).astype(jnp.bfloat16)
    sink_logits = sink_center + jax.random.normal(shared_keys[3], (Q_HEADS,), jnp.float32)
    w_o = (4.0 * (Q_HEADS * HEAD_DIM) ** -0.5 * jax.random.normal(shared_keys[4], (Q_HEADS * HEAD_DIM, D_MODEL), jnp.float32)).astype(jnp.bfloat16)
    b_o = (0.3 * jax.random.normal(shared_keys[5], (D_MODEL,), jnp.float32)).astype(jnp.bfloat16)
    return {"hidden": hidden, "seq_lens": seq_lens, "rope_cos": jnp.cos(angles), "rope_sin": jnp.sin(angles), "k_cache": k_cache, "v_cache": v_cache, "norm_gain": norm_gain, "w_qkv": w_qkv, "b_qkv": b_qkv, "sink_logits": sink_logits, "w_o": w_o, "b_o": b_o}


def reference(hidden, seq_lens, rope_cos, rope_sin, k_cache, v_cache, norm_gain, w_qkv, b_qkv, sink_logits, w_o, b_o):
    group_size = Q_HEADS // KV_HEADS
    x_wide = hidden.astype(jnp.float32)
    inv_rms = lax.rsqrt(jnp.mean(x_wide * x_wide, axis=-1, keepdims=True) + NORM_EPS)
    normed = (x_wide * inv_rms * norm_gain.astype(jnp.float32)).astype(jnp.bfloat16)
    qkv_all = jnp.dot(normed, w_qkv.reshape(D_MODEL, KV_HEADS * (group_size + 2) * HEAD_DIM), preferred_element_type=jnp.float32)
    qkv_all = (qkv_all + b_qkv.astype(jnp.float32).reshape(-1)).reshape(SEQ_COUNT, KV_HEADS, group_size + 2, HEAD_DIM)
    q_rot = rotate_half(qkv_all[:, :, :group_size], rope_cos[:, None, None, :], rope_sin[:, None, None, :]).astype(jnp.bfloat16)
    k_new = rotate_half(qkv_all[:, :, group_size], rope_cos[:, None, :], rope_sin[:, None, :]).astype(jnp.bfloat16)
    v_new = qkv_all[:, :, group_size + 1].astype(jnp.bfloat16)
    positions = jnp.arange(CTX_LEN)
    is_new = (positions[None, :] == seq_lens[:, None])[:, :, None, None]
    k_out = jnp.where(is_new, k_new[:, None], k_cache)
    v_out = jnp.where(is_new, v_new[:, None], v_cache)
    sink_kg = sink_logits.reshape(KV_HEADS, group_size)
    logit_scale = HEAD_DIM ** -0.5

    def one_sequence(per_seq):
        q_seq, k_seq, v_seq, len_seq = per_seq
        logits = jnp.einsum("kgd,lkd->kgl", q_seq.astype(jnp.float32), k_seq.astype(jnp.float32)) * logit_scale
        logits = jnp.where((positions <= len_seq)[None, None, :], logits, -jnp.inf)
        row_max = jnp.maximum(jnp.max(logits, axis=-1), sink_kg)
        weights = jnp.exp(logits - row_max[..., None])
        denominator = jnp.sum(weights, axis=-1) + jnp.exp(sink_kg - row_max)
        weighted = jnp.einsum("kgl,lkd->kgd", weights.astype(jnp.bfloat16).astype(jnp.float32), v_seq.astype(jnp.float32))
        return weighted / denominator[..., None]

    head_out = lax.map(one_sequence, (q_rot, k_out, v_out, seq_lens))
    attn_out = jnp.dot(head_out.astype(jnp.bfloat16).reshape(SEQ_COUNT, Q_HEADS * HEAD_DIM), w_o, preferred_element_type=jnp.float32)
    out_hidden = (x_wide + attn_out + b_o.astype(jnp.float32)).astype(jnp.bfloat16)
    return out_hidden, k_out, v_out
```

```python
import functools

import jax
import jax.numpy as jnp
from jax import lax
from jax.experimental import pallas as pl
from jax.experimental.pallas import tpu as pltpu
from jax.sharding import PartitionSpec as P

NORM_EPS = 1e-5
MESH = pl.DeviceIdType.MESH
F32 = jnp.float32
BF16 = jnp.bfloat16
VMEM = pltpu.VMEM
DMA = pltpu.SemaphoreType.DMA

B = 64
D = 8192
L = 64
HD = 128
G = 8
RD = 256
NB = D // RD
NC = 4
CB = B // NC
CR = CB * G
NSUB = 2
QW = 2048
UW = QW // NSUB
NU = NC * NSUB


def core_peer(sp):
    return sp + 1 - 2 * lax.rem(sp, 2)


def qkv_kernel(hid_ref, gain_ref, w_ref, b_ref, cos_ref, sin_ref, q_ref, kv_ref, wbuf, xexp, tot, wsem, ssem, rsem):
    sp = lax.axis_index("sp")
    core = lax.rem(sp, 2)
    base = core * 5

    def wcopy(c, ct):
        return pltpu.make_async_copy(
            w_ref.at[pl.ds(pl.multiple_of(c * RD, RD), RD), base + ct], wbuf.at[c, ct], wsem.at[c, ct])

    def start(c, carry):
        for ct in range(5):
            wcopy(c, ct).start()
        return carry

    lax.fori_loop(0, NB, start, 0)
    barrier = pltpu.get_barrier_semaphore()
    pl.semaphore_signal(barrier, inc=1, device_id={"sp": core_peer(sp)}, device_id_type=MESH)

    sq = jnp.zeros((B, 128), F32)
    for k in range(8):
        x = hid_ref[:, k * 1024:(k + 1) * 1024].astype(F32)
        x = x * x
        for j in range(8):
            sq = sq + x[:, j * 128:(j + 1) * 128]
    inv = lax.rsqrt(jnp.sum(sq, axis=-1, keepdims=True) / D + NORM_EPS)

    row = lax.broadcasted_iota(jnp.int32, (128, 256), 0)
    lane = lax.broadcasted_iota(jnp.int32, (128, 256), 1)
    spread = jnp.where(lax.div(lane, 2) == row, 1.0, 0.0).astype(BF16)
    even = lax.rem(lax.broadcasted_iota(jnp.int32, (B, 256), 1), 2) == 0

    def expand(k, carry):
        cols = pl.ds(pl.multiple_of(k * 128, 128), 128)
        wide = pl.ds(pl.multiple_of(k * 256, 256), 256)
        h = (hid_ref[:, cols].astype(F32) * inv * gain_ref[:, cols].astype(F32)).astype(BF16)
        t = jnp.dot(h, spread, preferred_element_type=F32)
        xexp[:B, wide] = jnp.where(even, t, 0.0).astype(BF16)
        xexp[B:, wide] = jnp.where(even, 0.0, t).astype(BF16)
        return carry

    lax.fori_loop(0, D // 128, expand, 0, unroll=4)

    tot[pl.ds(base, 5)] = jnp.zeros((5, 2 * B, HD), F32)

    def block(c, carry):
        for ct in range(5):
            wcopy(c, ct).wait()
        w = jnp.concatenate([wbuf.at[c, ct].reshape(2 * RD, HD)[...] for ct in range(5)], axis=1)
        wide = pl.ds(pl.multiple_of(c * 2 * RD, 2 * RD), 2 * RD)
        r = jnp.dot(xexp[:, wide], w, preferred_element_type=F32)
        for ct in range(5):
            tot[base + ct] += r[:, ct * HD:(ct + 1) * HD]
        return carry

    lax.fori_loop(0, NB, block, 0)
    pl.semaphore_wait(barrier, 1)
    copy = pltpu.make_async_remote_copy(
        src_ref=tot.at[pl.ds(base, 5)], dst_ref=tot.at[pl.ds(base, 5)], send_sem=ssem, recv_sem=rsem,
        device_id={"sp": core_peer(sp)}, device_id_type=MESH)
    copy.start()
    cos, sin = cos_ref[...], sin_ref[...]
    cos2 = jnp.concatenate([cos, cos], axis=1)
    sin2 = jnp.concatenate([-sin, sin], axis=1)
    bias = b_ref[...].astype(F32)
    copy.wait()
    for ct in range(10):
        for h in range(2):
            t = tot[ct, h * B:(h + 1) * B, :] + bias[h:h + 1, ct * HD:(ct + 1) * HD]
            if ct < 9:
                t = t * cos2 + pltpu.roll(t, 64, 1) * sin2
            t = t.astype(BF16).astype(F32)
            if ct < G:
                q_ref[h, pl.ds(ct, B, stride=G), :] = t
            else:
                kv_ref[ct - G, h] = t


def attend_kernel(q_ref, kv_ref, kc_ref, vc_ref, len_ref, sink_ref, ko_ref, vo_ref, n_ref, kbuf, vbuf, isem, osem):
    sp = lax.axis_index("sp")

    def load(src, dst, which, i):
        s = pl.ds(i * CB, CB)
        return pltpu.make_async_copy(src.at[s], dst.at[s], isem.at[which, i])

    def save(src, dst, which, i):
        s = pl.ds(i * CB, CB)
        return pltpu.make_async_copy(src.at[s], dst.at[s], osem.at[which, i])

    for i in range(NC):
        load(kc_ref, kbuf, 0, i).start()
        load(vc_ref, vbuf, 1, i).start()

    sub = lax.broadcasted_iota(jnp.int32, (G, HD), 0)
    lane = lax.broadcasted_iota(jnp.int32, (G, HD), 1)
    pos = lax.div(lane, 2)
    par = lax.rem(lane, 2)
    sinks = []
    for h in range(2):
        t = jnp.zeros((G, HD), F32)
        for g in range(G):
            t = jnp.where(sub == g, sink_ref[h * G + g], t)
        sinks.append(t)
    eye = lax.broadcasted_iota(jnp.int32, (CR, HD), 0) == lax.broadcasted_iota(jnp.int32, (CR, HD), 1)
    scale = HD ** -0.5

    def chunk(i, carry):
        load(kc_ref, kbuf, 0, i).wait()
        load(vc_ref, vbuf, 1, i).wait()
        locs = []
        for j in range(CB):
            b = i * CB + j
            loc = len_ref[b] - sp * L
            locs.append(loc)

            @pl.when((loc >= 0) & (loc < L))
            def _():
                for which, buf in ((0, kbuf), (1, vbuf)):
                    pair = jnp.concatenate([kv_ref[which, 0, pl.ds(b, 1), :], kv_ref[which, 1, pl.ds(b, 1), :]], axis=0)
                    buf[b, loc] = pair.astype(BF16)

        save(kbuf, ko_ref, 0, i).start()
        save(vbuf, vo_ref, 1, i).start()
        s0, s1 = [], []
        for j in range(CB):
            b = i * CB + j
            rows = pl.ds(pl.multiple_of(b * G, G), G)
            q = jnp.concatenate([q_ref[0, rows, :], q_ref[1, rows, :]], axis=0).astype(BF16)
            k = kbuf.at[b].reshape(2 * L, HD)[...]
            s = lax.dot_general(q, k, (((1,), (1,)), ((), ())), preferred_element_type=F32) * scale
            seen = pos <= locs[j]
            s0.append(jnp.where(seen & (par == 0), s[:G], -jnp.inf))
            s1.append(jnp.where(seen & (par == 1), s[G:], -jnp.inf))
        es = []
        for h, parts in ((0, s0), (1, s1)):
            s = jnp.concatenate(parts, axis=0)
            m = jnp.maximum(jnp.max(s, axis=-1, keepdims=True), jnp.concatenate([sinks[h][:, :1]] * CB, axis=0))
            e = jnp.exp(s - m)
            z = jnp.sum(e, axis=-1, keepdims=True)
            es.append(e)
            mrow = jnp.sum(jnp.where(eye, m, 0.0), axis=0, keepdims=True)
            zrow = jnp.sum(jnp.where(eye, z, 0.0), axis=0, keepdims=True)
            n_ref[i, h, CR:, :] = jnp.concatenate([mrow, zrow, jnp.zeros((6, HD), F32)], axis=0)
        for j in range(CB):
            b = i * CB + j
            e = jnp.concatenate([es[0][j * G:(j + 1) * G], es[1][j * G:(j + 1) * G]], axis=0).astype(BF16)
            v = vbuf.at[b].reshape(2 * L, HD)[...]
            r = jnp.dot(e, v, preferred_element_type=F32)
            n_ref[i, 0, j * G:(j + 1) * G, :] = r[:G]
            n_ref[i, 1, j * G:(j + 1) * G, :] = r[G:]
        return carry

    lax.fori_loop(0, NC, chunk, 0)
    for i in range(NC):
        save(kbuf, ko_ref, 0, i).wait()
        save(vbuf, vo_ref, 1, i).wait()


def out_kernel(n_ref, hid_ref, wo_ref, bo_ref, sink_ref, y_ref, wo, r1, comb, r2, obuf, part, near, both, other, full,
               wsem, s1, q1, s2, q2, s3, q3, sn, qn, sm, qm, sf, qf, sy, qy, sc, qc, sd, qd):
    sp = lax.axis_index("sp")
    z = lax.axis_index("tp")
    core = lax.rem(sp, 2)
    peer = core_peer(sp)
    ypeer = lax.rem(sp + 2, 4)
    zpeer = z + 1 - 2 * lax.rem(z, 2)
    zmid = 3 - z
    middle = (z == 1) | (z == 2)
    end = (z == 0) | (z == 3)

    def wcopy(k):
        rows = pl.ds(k * 512, 512)
        return pltpu.make_async_copy(
            wo_ref.at[rows, pl.ds(pl.multiple_of(sp * QW, QW), QW)], wo.at[rows], wsem.at[k])

    for k in range(4):
        wcopy(k).start()
    barrier = pltpu.get_barrier_semaphore()
    pl.semaphore_signal(barrier, inc=1, device_id={"sp": peer}, device_id_type=MESH)
    pl.semaphore_signal(barrier, inc=1, device_id={"sp": ypeer}, device_id_type=MESH)
    pl.semaphore_signal(barrier, inc=1, device_id={"tp": zpeer}, device_id_type=MESH)

    @pl.when(middle)
    def _():
        pl.semaphore_signal(barrier, inc=1, device_id={"tp": zmid}, device_id_type=MESH)
        pl.semaphore_wait(barrier, 4)

    @pl.when(end)
    def _():
        pl.semaphore_wait(barrier, 3)

    def remote(src, dst, send, recv, axis, target):
        return pltpu.make_async_remote_copy(
            src_ref=src, dst_ref=dst, send_sem=send, recv_sem=recv, device_id={axis: target}, device_id_type=MESH)

    def c_swap(i):
        return remote(n_ref.at[i, 1 - core], r1.at[i], s1.at[i], q1.at[i], "sp", peer)

    def c_y(i):
        return remote(comb.at[i], r2.at[i], s2.at[i], q2.at[i], "sp", ypeer)

    def c_o(i):
        return remote(obuf.at[core, i], obuf.at[core, i], s3.at[i], q3.at[i], "sp", peer)

    def c_near(u):
        return remote(part.at[u], near.at[u], sn.at[u], qn.at[u], "tp", zpeer)

    def c_mid(u):
        return remote(both.at[u], other.at[u], sm.at[u], qm.at[u], "tp", zmid)

    def c_full(u):
        return remote(full.at[sp, u], full.at[sp, u], sf.at[u], qf.at[u], "tp", zpeer)

    def c_fy(u):
        return remote(full.at[sp, u], full.at[sp, u], sy.at[u], qy.at[u], "sp", ypeer)

    def c_fc(u):
        return remote(full.at[sp, u], full.at[sp, u], sc.at[u], qc.at[u], "sp", peer)

    def c_fd(u):
        return remote(full.at[ypeer, u], full.at[ypeer, u], sd.at[u], qd.at[u], "sp", peer)

    for i in range(NC):
        c_swap(i).start()

    eye = lax.broadcasted_iota(jnp.int32, (CR, HD), 0) == lax.broadcasted_iota(jnp.int32, (CR, HD), 1)

    def column(r):
        return jnp.sum(jnp.where(eye, r, 0.0), axis=-1, keepdims=True)

    lane = lax.broadcasted_iota(jnp.int32, (1, HD), 1)
    sink = jnp.zeros((1, HD), F32)
    for g in range(G):
        sink = jnp.where(lax.rem(lane, G) == g, sink_ref[core * G + g], sink)

    for i in range(NC):
        c_swap(i).wait_recv()
        m1, m2 = n_ref[i, core, CR:CR + 1, :], r1[i, CR:CR + 1, :]
        z1, z2 = n_ref[i, core, CR + 1:CR + 2, :], r1[i, CR + 1:CR + 2, :]
        m = jnp.maximum(m1, m2)
        a1, a2 = jnp.exp(m1 - m), jnp.exp(m2 - m)
        comb[i, :CR, :] = n_ref[i, core, :CR, :] * column(a1) + r1[i, :CR, :] * column(a2)
        comb[i, CR:, :] = jnp.concatenate([m, z1 * a1 + z2 * a2, jnp.zeros((6, HD), F32)], axis=0)
        c_y(i).start()

    def project(i):
        c_y(i).wait_recv()
        m1, m2 = comb[i, CR:CR + 1, :], r2[i, CR:CR + 1, :]
        z1, z2 = comb[i, CR + 1:CR + 2, :], r2[i, CR + 1:CR + 2, :]
        m = jnp.maximum(m1, m2)
        a1, a2 = jnp.exp(m1 - m), jnp.exp(m2 - m)
        den = z1 * a1 + z2 * a2 + jnp.exp(sink - m)
        o = comb[i, :CR, :] * column(a1 / den) + r2[i, :CR, :] * column(a2 / den)
        obuf[core, i] = o.astype(BF16).astype(F32)
        c_o(i).start()
        if i == 0:
            for k in range(4):
                wcopy(k).wait()
        c_o(i).wait_recv()
        lhs = jnp.concatenate(
            [obuf[h, i, pl.ds(g, CB, stride=G), :] for h in range(2) for g in range(G)], axis=1).astype(BF16)
        for s in range(NSUB):
            def tile(t, carry):
                cols = pl.ds(pl.multiple_of(s * UW + t * 256, 256), 256)
                part[i * NSUB + s, :, pl.ds(pl.multiple_of(t * 256, 256), 256)] = jnp.dot(
                    lhs, wo[:, cols], preferred_element_type=F32)
                return carry
            lax.fori_loop(0, UW // 256, tile, 0)

            @pl.when(end)
            def _():
                c_near(i * NSUB + s).start()

    def gather(u):
        c_fy(u).start()
        c_fc(u).start()

    def first(u):
        @pl.when(middle)
        def _():
            c_near(u).wait_recv()
            both[u] = part[u] + near[u]
            c_mid(u).start()

    def second(u):
        @pl.when(middle)
        def _():
            c_mid(u).wait_recv()
            full[sp, u] = both[u] + other[u]
            c_full(u).start()
            gather(u)

    def third(u):
        @pl.when(end)
        def _():
            c_full(u).wait_recv()
            gather(u)

    def fourth(u):
        c_fy(u).wait_recv()
        c_fd(u).start()

    def last(u):
        c_fc(u).wait_recv()
        c_fd(u).wait_recv()
        i, s = u // NSUB, u % NSUB
        for k in range(4):
            cols = pl.ds(k * QW + s * UW, UW)
            rows = pl.ds(i * CB, CB)
            y_ref[rows, cols] = (hid_ref[rows, cols].astype(F32) + full[k, u] + bo_ref[:, cols].astype(F32)).astype(BF16)

    stages = ((first, 2), (second, 4), (third, 5), (fourth, 6), (last, 8))
    for t in range(NU + 8):
        if t % NSUB == 0 and t < NU:
            project(t // NSUB)
        for stage, lag in stages:
            if 0 <= t - lag < NU:
                stage(t - lag)

    for i in range(NC):
        c_swap(i).wait_send()
        c_y(i).wait_send()
        c_o(i).wait_send()
    for u in range(NU):
        c_fy(u).wait_send()
        c_fc(u).wait_send()
        c_fd(u).wait_send()

    @pl.when(middle)
    def _():
        for u in range(NU):
            c_mid(u).wait_send()
            c_full(u).wait_send()

    @pl.when(end)
    def _():
        for u in range(NU):
            c_near(u).wait_send()


def vm():
    return pl.BlockSpec(memory_space=VMEM)


def anywhere():
    return pl.BlockSpec(memory_space=pl.ANY)


def smem():
    return pl.BlockSpec(memory_space=pltpu.SMEM)


def solution(mesh):
    cache_spec = P("dp", "sp", "tp", None)

    def step(hidden, seq_lens, rope_cos, rope_sin, k_cache, v_cache, norm_gain, w_qkv, b_qkv, sink_logits, w_o, b_o):
        w_tiles = w_qkv.reshape(D, 2, 10, HD).transpose(0, 2, 1, 3)
        q, kv = pl.pallas_call(
            qkv_kernel,
            name="qkv",
            out_shape=(jax.ShapeDtypeStruct((2, B * G, HD), F32), jax.ShapeDtypeStruct((2, 2, B, HD), F32)),
            in_specs=[vm(), vm(), anywhere(), vm(), vm(), vm()],
            out_specs=(vm(), vm()),
            scratch_shapes=[
                VMEM((NB, 5, RD, 2, HD), BF16), VMEM((2 * B, 2 * D), BF16), VMEM((10, 2 * B, HD), F32),
                DMA((NB, 5)), DMA, DMA],
            compiler_params=pltpu.CompilerParams(
                collective_id=0, has_side_effects=True, vmem_limit_bytes=40 * 2**20),
        )(hidden, norm_gain.reshape(1, D), w_tiles, b_qkv, rope_cos, rope_sin)
        k_out, v_out, num = pl.pallas_call(
            attend_kernel,
            name="attend",
            out_shape=(jax.ShapeDtypeStruct((B, L, 2, HD), BF16), jax.ShapeDtypeStruct((B, L, 2, HD), BF16),
                       jax.ShapeDtypeStruct((NC, 2, CR + 8, HD), F32)),
            in_specs=[vm(), vm(), anywhere(), anywhere(), smem(), smem()],
            out_specs=(anywhere(), anywhere(), vm()),
            scratch_shapes=[VMEM((B, L, 2, HD), BF16), VMEM((B, L, 2, HD), BF16), DMA((2, NC)), DMA((2, NC))],
            compiler_params=pltpu.CompilerParams(vmem_limit_bytes=24 * 2**20),
        )(q, kv, k_cache, v_cache, seq_lens, sink_logits)
        unit = (NU, CB, UW)
        out_hidden = pl.pallas_call(
            out_kernel,
            name="out",
            out_shape=jax.ShapeDtypeStruct((B, D), BF16),
            in_specs=[vm(), vm(), anywhere(), vm(), smem()],
            out_specs=vm(),
            scratch_shapes=[
                VMEM((2048, QW), BF16),
                VMEM((NC, CR + 8, HD), F32), VMEM((NC, CR + 8, HD), F32), VMEM((NC, CR + 8, HD), F32),
                VMEM((2, NC, CR, HD), F32),
                VMEM(unit, F32), VMEM(unit, F32), VMEM(unit, F32), VMEM(unit, F32), VMEM((4, *unit), F32),
                DMA((4,))] + [DMA((NC,))] * 6 + [DMA((NU,))] * 12,
            compiler_params=pltpu.CompilerParams(
                collective_id=1, has_side_effects=True, vmem_limit_bytes=32 * 2**20),
        )(num, hidden, w_o, b_o.reshape(1, D), sink_logits)
        return out_hidden, k_out, v_out

    return jax.shard_map(
        step, mesh=mesh,
        in_specs=(P("dp", None), P("dp"), P("dp", None), P("dp", None), cache_spec, cache_spec, P(None),
                  P(None, "tp", None), P("tp", None), P("tp"), P("tp", None), P(None)),
        out_specs=(P("dp", None), cache_spec, cache_spec), check_vma=False)
```
